8 devices in a mesh: dp: 2 (over z, y), cp: 4 (over x, core).
Axes of the slice: x: 2, y: 2, z: 1, core: 2. Of those that a mesh axis runs over, the one named last changes fastest.
Arguments:
- x_act: bfloat16 [16, 1024, 2048], P('dp', 'cp')
- d_out: bfloat16 [16, 1024, 2048], P('dp', 'cp')
- seg_ids: int32 [16, 1024], P('dp', 'cp')
- w_q: bfloat16 [2048, 16, 128], replicated
- w_k: bfloat16 [2048, 2, 128], replicated
- w_v: bfloat16 [2048, 2, 128], replicated
- w_o: bfloat16 [16, 128, 2048], replicated
- w_up: bfloat16 [2048, 11008], replicated
- w_down: bfloat16 [11008, 2048], replicated
Outputs:
- output 1: bfloat16 [16, 1024, 2048], P('dp', 'cp')
- output 2: float32 [2048, 16, 128], replicated
- output 3: float32 [2048, 2, 128], replicated
- output 4: float32 [2048, 2, 128], replicated
- output 5: float32 [16, 128, 2048], replicated
- output 6: float32 [2048, 11008], replicated
- output 7: float32 [11008, 2048], replicated
All inputs are finite; a program needn't handle non-finite values.
Results may differ from the reference program's by a relative error of at most 0.0165975.
Values are sent between devices in bfloat16 or wider.
A program may use at most 1.5 GiB of HBM per device.

```python
import jax
import jax.numpy as jnp
from jax import lax

MODEL_DIM = 2048
HEADS = 16
KV_HEADS = 2
HEAD_DIM = 128
FFN_DIM = 11008
BATCH = 16
SEQ_LEN = 1024
CP_SIZE = 4
WORKERS = 8
NUM_DOCS = 4

GROUP_SIZE = HEADS // KV_HEADS
PIECE_LEN = SEQ_LEN // (2 * CP_SIZE)
SCORE_SCALE = HEAD_DIM ** -0.5


def bf16_value(val_in):
    return val_in + lax.stop_gradient(val_in.astype(jnp.bfloat16).astype(jnp.float32) - val_in)


def to_true_order(array_in):
    shaped = array_in.reshape((array_in.shape[0], CP_SIZE, 2, PIECE_LEN) + array_in.shape[2:])
    front_part = shaped[:, :, 0]
    back_part = jnp.flip(shaped[:, :, 1], axis=1)
    return jnp.concatenate([front_part, back_part], axis=1).reshape(array_in.shape)


def to_stored_order(array_in):
    shaped = array_in.reshape((array_in.shape[0], 2, CP_SIZE, PIECE_LEN) + array_in.shape[2:])
    front_part = shaped[:, 0]
    back_part = jnp.flip(shaped[:, 1], axis=1)
    return jnp.stack([front_part, back_part], axis=2).reshape(array_in.shape)


def draw_weight(rng_key, arr_shape, std_dev):
    return (jax.random.normal(rng_key, arr_shape, jnp.float32) * std_dev).astype(jnp.bfloat16)


def setup_inputs(seed: int = 0) -> dict:
    keys = jax.random.split(jax.random.key(seed), 9)
    attn_gain = (SEQ_LEN / (8.0 * NUM_DOCS)) ** 0.5
    qk_std = 0.7 * MODEL_DIM ** -0.5
    x_act = jax.random.normal(keys[0], (BATCH, SEQ_LEN, MODEL_DIM), jnp.float32)
    d_out = jax.random.normal(keys[1], (BATCH, SEQ_LEN, MODEL_DIM), jnp.float32)
    cut_points = jnp.sort(jax.random.randint(keys[2], (BATCH, NUM_DOCS - 1), 1, SEQ_LEN), axis=1)
    positions = jnp.arange(SEQ_LEN, dtype=jnp.int32)
    seg_true = jnp.sum((positions[None, :, None] >= cut_points[:, None, :]).astype(jnp.int32), axis=2)
    return {
        'x_act': x_act.astype(jnp.bfloat16),
        'd_out': d_out.astype(jnp.bfloat16),
        'seg_ids': to_stored_order(seg_true).astype(jnp.int32),
        'w_q': draw_weight(keys[3], (MODEL_DIM, HEADS, HEAD_DIM), qk_std),
        'w_k': draw_weight(keys[4], (MODEL_DIM, KV_HEADS, HEAD_DIM), qk_std),
        'w_v': draw_weight(keys[5], (MODEL_DIM, KV_HEADS, HEAD_DIM), MODEL_DIM ** -0.5),
        'w_o': draw_weight(keys[6], (HEADS, HEAD_DIM, MODEL_DIM), attn_gain * (HEADS * HEAD_DIM) ** -0.5),
        'w_up': draw_weight(keys[7], (MODEL_DIM, FFN_DIM), MODEL_DIM ** -0.5),
        'w_down': draw_weight(keys[8], (FFN_DIM, MODEL_DIM), FFN_DIM ** -0.5),
    }


def layer_one(x_seq, seg_seq, q_weight, k_weight, v_weight, o_weight, up_weight, down_weight):
    queries = bf16_value(jnp.einsum('sd,dnk->snk', x_seq, q_weight)).reshape(SEQ_LEN // PIECE_LEN, PIECE_LEN, KV_HEADS, GROUP_SIZE, HEAD_DIM)
    key_act = bf16_value(jnp.einsum('sd,dnk->snk', x_seq, k_weight))
    value_act = bf16_value(jnp.einsum('sd,dnk->snk', x_seq, v_weight))
    positions = jnp.arange(SEQ_LEN)

    def block_attention(block_in):
        q_blk, q_seg, q_pos = block_in
        scores = jnp.einsum('qngk,tnk->ngqt', q_blk, key_act) * SCORE_SCALE
        allowed = (q_pos[:, None] >= positions[None, :]) & (q_seg[:, None] == seg_seq[None, :])
        scores = jnp.where(allowed[None, None], scores, -1e30)
        probs_row = bf16_value(jax.nn.softmax(scores, axis=-1))
        return jnp.einsum('ngqt,tnk->qngk', probs_row, value_act)

    attn_out = lax.map(jax.checkpoint(block_attention), (queries, seg_seq.reshape(-1, PIECE_LEN), positions.reshape(-1, PIECE_LEN)))
    attn_out = bf16_value(attn_out.reshape(SEQ_LEN, HEADS, HEAD_DIM))
    hidden = bf16_value(x_seq + jnp.einsum('snk,nkd->sd', attn_out, o_weight))
    act_out = bf16_value(jax.nn.gelu(jnp.dot(hidden, up_weight), approximate=True))
    return hidden + jnp.dot(act_out, down_weight)


def reference(x_act, d_out, seg_ids, w_q, w_k, w_v, w_o, w_up, w_down):
    weights = tuple(weight.astype(jnp.float32) for weight in (w_q, w_k, w_v, w_o, w_up, w_down))
    x_true = to_true_order(x_act).astype(jnp.float32)
    dout_true = to_true_order(d_out).astype(jnp.float32)
    seg_true = to_true_order(seg_ids)

    def one_sequence(grad_sums, seq_data):
        x_seq, dout_seq, seg_seq = seq_data

        def layer_fn(x_in, q_weight, k_weight, v_weight, o_weight, up_weight, down_weight):
            return layer_one(x_in, seg_seq, q_weight, k_weight, v_weight, o_weight, up_weight, down_weight)

        _, pullback = jax.vjp(layer_fn, x_seq, *weights)
        cotangents = pullback(dout_seq)
        new_sums = tuple(sum_prev + part_grad for sum_prev, part_grad in zip(grad_sums, cotangents[1:]))
        return new_sums, cotangents[0]

    zero_sums = tuple(jnp.zeros_like(weight) for weight in weights)
    grad_sums, dx_true = lax.scan(one_sequence, zero_sums, (x_true, dout_true, seg_true))
    d_x = to_stored_order(dx_true).astype(jnp.bfloat16)
    return (d_x, grad_sums[0] / WORKERS, grad_sums[1] / WORKERS, grad_sums[2] / WORKERS, grad_sums[3] / WORKERS, grad_sums[4] / WORKERS, grad_sums[5] / WORKERS)
```

```python
import jax
import jax.numpy as jnp
from jax import lax
from jax.experimental import pallas as pl
from jax.experimental.pallas import tpu as pltpu
from jax.sharding import PartitionSpec as P

NEG_BIG = -1e30
PIECE = 128
KV_BLOCK = 256
LANE = 128


NT = (((1,), (1,)), ((), ()))
NN = (((1,), (0,)), ((), ()))
TN = (((0,), (0,)), ((), ()))


def mm(lhs, rhs, dims=NN):
    return lax.dot_general(lhs, rhs, dims, preferred_element_type=jnp.float32)


def gelu_tanh(pre_act):
    return jax.nn.gelu(pre_act, approximate=True)


def order_pieces(cp_size):
    return [(t, 0) if t < cp_size else (2 * cp_size - 1 - t, 1) for t in range(2 * cp_size)]


def piece_bounds(scal_ref, piece_idx, batch_idx, cp_size):
    cp_index = scal_ref[0]
    piece = cp_index if piece_idx == 0 else 2 * cp_size - 1 - cp_index
    low = scal_ref[1 + 2 * batch_idx + piece_idx]
    return piece, low, (piece + 2) // 2


def block_mask(kv_start, start_row, pos_row):
    kv_pos = kv_start + lax.broadcasted_iota(jnp.int32, (KV_BLOCK, 2 * PIECE), 0)
    return (kv_pos >= start_row) & (kv_pos <= pos_row)


def rows_of(start_ref, piece_idx, piece):
    part = start_ref[0, :, piece_idx * PIECE:(piece_idx + 1) * PIECE]
    start_row = jnp.concatenate([part, part], axis=1)
    pos_row = piece * PIECE + lax.rem(lax.broadcasted_iota(jnp.int32, (1, 2 * PIECE), 1), PIECE)
    return start_row, pos_row


def attn_forward_kernel(cp_size, group, scale, scal_ref, q_ref, k_ref, v_ref, start_ref, o_ref, lse_ref, k_scr, v_scr, q_scr, s_scr, acc_scr):
    batch_idx = pl.program_id(0)
    for t, (dev, half) in enumerate(order_pieces(cp_size)):
        k_scr[t * PIECE:(t + 1) * PIECE, :] = k_ref[dev, 0, half * PIECE:(half + 1) * PIECE, :]
        v_scr[t * PIECE:(t + 1) * PIECE, :] = v_ref[dev, 0, half * PIECE:(half + 1) * PIECE, :]
    width = group * PIECE
    pairs = group // 2
    for piece_idx in range(2):
        piece, low, high = piece_bounds(scal_ref, piece_idx, batch_idx, cp_size)
        rows = slice(piece_idx * PIECE, (piece_idx + 1) * PIECE)
        for head in range(group):
            q_scr[head * PIECE:(head + 1) * PIECE, :] = q_ref[0, rows, head * LANE:(head + 1) * LANE]
        start_row, pos_row = rows_of(start_ref, piece_idx, piece)

        def score_step(blk, row_max):
            at = pl.multiple_of(blk * KV_BLOCK, KV_BLOCK)
            k_blk = k_scr[pl.ds(at, KV_BLOCK), :]
            allowed = block_mask(at, start_row, pos_row)
            new_max = []
            for pair in range(pairs):
                cols = slice(pair * 2 * PIECE, (pair + 1) * 2 * PIECE)
                scores = mm(k_blk, q_scr[cols, :], NT) * scale
                scores = jnp.where(allowed, scores, NEG_BIG)
                s_scr[pl.ds(at, KV_BLOCK), cols] = scores
                new_max.append(jnp.maximum(row_max[pair], jnp.max(scores, axis=0, keepdims=True)))
            return tuple(new_max)

        row_max = lax.fori_loop(low, high, score_step, tuple(jnp.full((1, 2 * PIECE), NEG_BIG, jnp.float32) for _ in range(pairs)))
        acc_scr[...] = jnp.zeros((LANE, width), jnp.float32)

        def value_step(blk, row_sum):
            at = pl.multiple_of(blk * KV_BLOCK, KV_BLOCK)
            v_blk = v_scr[pl.ds(at, KV_BLOCK), :]
            new_sum = []
            for pair in range(pairs):
                cols = slice(pair * 2 * PIECE, (pair + 1) * 2 * PIECE)
                exp_scores = jnp.exp(s_scr[pl.ds(at, KV_BLOCK), cols] - row_max[pair])
                new_sum.append(row_sum[pair] + jnp.sum(exp_scores, axis=0, keepdims=True))
                acc_scr[:, cols] += mm(v_blk, exp_scores.astype(jnp.bfloat16), TN)
            return tuple(new_sum)

        row_sum = lax.fori_loop(low, high, value_step, tuple(jnp.zeros((1, 2 * PIECE), jnp.float32) for _ in range(pairs)))
        for pair in range(pairs):
            cols = slice(pair * 2 * PIECE, (pair + 1) * 2 * PIECE)
            lse_ref[0, 0, piece_idx:piece_idx + 1, cols] = row_max[pair] + jnp.log(row_sum[pair])
            out = jnp.transpose(acc_scr[:, cols] / row_sum[pair]).astype(jnp.bfloat16)
            for side in range(2):
                head = 2 * pair + side
                o_ref[0, rows, head * LANE:(head + 1) * LANE] = out[side * PIECE:(side + 1) * PIECE, :]


def attn_backward_kernel(cp_size, group, scale, scal_ref, q_ref, k_ref, v_ref, start_ref, o_ref, do_ref, lse_ref, dq_ref, dk_ref, dv_ref,
                         k_scr, v_scr, q_scr, do_scr, dqt_scr, dk_scr, dv_scr):
    batch_idx = pl.program_id(0)
    for t, (dev, half) in enumerate(order_pieces(cp_size)):
        k_scr[t * PIECE:(t + 1) * PIECE, :] = k_ref[dev, 0, half * PIECE:(half + 1) * PIECE, :]
        v_scr[t * PIECE:(t + 1) * PIECE, :] = v_ref[dev, 0, half * PIECE:(half + 1) * PIECE, :]
    dk_scr[...] = jnp.zeros(dk_scr.shape, jnp.float32)
    dv_scr[...] = jnp.zeros(dv_scr.shape, jnp.float32)
    pairs = group // 2
    for piece_idx in range(2):
        piece, low, high = piece_bounds(scal_ref, piece_idx, batch_idx, cp_size)
        rows = slice(piece_idx * PIECE, (piece_idx + 1) * PIECE)
        start_row, pos_row = rows_of(start_ref, piece_idx, piece)
        deltas = []
        for head in range(group):
            lanes = slice(head * LANE, (head + 1) * LANE)
            d_out = do_ref[0, rows, lanes]
            q_scr[head * PIECE:(head + 1) * PIECE, :] = q_ref[0, rows, lanes]
            do_scr[head * PIECE:(head + 1) * PIECE, :] = d_out
            prod = d_out.astype(jnp.float32) * o_ref[0, rows, lanes].astype(jnp.float32)
            deltas.append(jnp.sum(jnp.transpose(prod), axis=0, keepdims=True))
        delta_rows = [jnp.concatenate(deltas[2 * pair:2 * pair + 2], axis=1) for pair in range(pairs)]
        dqt_scr[...] = jnp.zeros(dqt_scr.shape, jnp.float32)

        def step(blk, carry):
            at = pl.multiple_of(blk * KV_BLOCK, KV_BLOCK)
            k_blk = k_scr[pl.ds(at, KV_BLOCK), :]
            v_blk = v_scr[pl.ds(at, KV_BLOCK), :]
            allowed = block_mask(at, start_row, pos_row)
            dk_sum = dk_scr[pl.ds(at, KV_BLOCK), :]
            dv_sum = dv_scr[pl.ds(at, KV_BLOCK), :]
            for pair in range(pairs):
                cols = slice(pair * 2 * PIECE, (pair + 1) * 2 * PIECE)
                q_pair = q_scr[cols, :]
                do_pair = do_scr[cols, :]
                scores = mm(k_blk, q_pair, NT) * scale
                prob = jnp.where(allowed, jnp.exp(scores - lse_ref[0, 0, piece_idx:piece_idx + 1, cols]), 0.0)
                d_prob = mm(v_blk, do_pair, NT)
                d_score = (prob * (d_prob - delta_rows[pair]) * scale).astype(jnp.bfloat16)
                dv_sum = dv_sum + mm(prob.astype(jnp.bfloat16), do_pair)
                dk_sum = dk_sum + mm(d_score, q_pair)
                dqt_scr[:, cols] += mm(k_blk, d_score, TN)
            dk_scr[pl.ds(at, KV_BLOCK), :] = dk_sum
            dv_scr[pl.ds(at, KV_BLOCK), :] = dv_sum
            return carry

        lax.fori_loop(low, high, step, 0)
        for pair in range(pairs):
            cols = slice(pair * 2 * PIECE, (pair + 1) * 2 * PIECE)
            d_q = jnp.transpose(dqt_scr[:, cols]).astype(jnp.bfloat16)
            for side in range(2):
                head = 2 * pair + side
                dq_ref[0, rows, head * LANE:(head + 1) * LANE] = d_q[side * PIECE:(side + 1) * PIECE, :]
    for t, (dev, half) in enumerate(order_pieces(cp_size)):
        dk_ref[dev, 0, half * PIECE:(half + 1) * PIECE, :] = dk_scr[t * PIECE:(t + 1) * PIECE, :]
        dv_ref[dev, 0, half * PIECE:(half + 1) * PIECE, :] = dv_scr[t * PIECE:(t + 1) * PIECE, :]


def attention(mode, cp_size, group, kv_heads, scale, scal, queries, kv_all, start, extra=()):
    batch, seq_local, width = queries.shape
    seq_len = cp_size * seq_local
    gw = group * LANE
    kernel = attn_forward_kernel if mode == "forward" else attn_backward_kernel
    q_spec = pl.BlockSpec((1, seq_local, gw), lambda b, n, s: (b, 0, n))
    k_spec = pl.BlockSpec((cp_size, 1, seq_local, LANE), lambda b, n, s: (0, b, 0, n))
    v_spec = pl.BlockSpec((cp_size, 1, seq_local, LANE), lambda b, n, s: (0, b, 0, kv_heads + n))
    start_spec = pl.BlockSpec((1, 1, seq_local), lambda b, n, s: (b, 0, 0))
    lse_spec = pl.BlockSpec((1, 1, 2, group * PIECE), lambda b, n, s: (b, n, 0, 0))
    act_shape = jax.ShapeDtypeStruct(queries.shape, jnp.bfloat16)
    bf = jnp.bfloat16
    f32 = jnp.float32
    flops = 2 * batch * kv_heads * group * seq_local * (seq_len // 2 + PIECE) * LANE
    if mode == "forward":
        in_specs = [q_spec, k_spec, v_spec, start_spec]
        out_specs = [q_spec, lse_spec]
        out_shape = [act_shape, jax.ShapeDtypeStruct((batch, kv_heads, 2, group * PIECE), f32)]
        scratch = [pltpu.VMEM((seq_len, LANE), bf), pltpu.VMEM((seq_len, LANE), bf), pltpu.VMEM((group * PIECE, LANE), bf),
                   pltpu.VMEM((seq_len, group * PIECE), f32), pltpu.VMEM((LANE, group * PIECE), f32)]
        flops = 4 * flops
    else:
        in_specs = [q_spec, k_spec, v_spec, start_spec, q_spec, q_spec, lse_spec]
        kv_out = jax.ShapeDtypeStruct((cp_size, batch, seq_local, kv_heads * LANE), f32)
        out_specs = [q_spec, k_spec, k_spec]
        out_shape = [act_shape, kv_out, kv_out]
        scratch = [pltpu.VMEM((seq_len, LANE), bf), pltpu.VMEM((seq_len, LANE), bf), pltpu.VMEM((group * PIECE, LANE), bf),
                   pltpu.VMEM((group * PIECE, LANE), bf), pltpu.VMEM((LANE, group * PIECE), f32),
                   pltpu.VMEM((seq_len, LANE), f32), pltpu.VMEM((seq_len, LANE), f32)]
        flops = 8 * flops

    def body(*refs):
        kernel(cp_size, group, scale, *refs)

    return pl.pallas_call(
        body,
        grid_spec=pltpu.PrefetchScalarGridSpec(num_scalar_prefetch=1, grid=(batch, kv_heads), in_specs=in_specs, out_specs=out_specs, scratch_shapes=scratch),
        out_shape=out_shape,
        compiler_params=pltpu.CompilerParams(vmem_limit_bytes=48 * 1024 * 1024),
        cost_estimate=pl.CostEstimate(flops=flops, bytes_accessed=40 * 1024 * 1024, transcendentals=flops // 512),
        name="attn_" + mode,
    )(scal, queries, kv_all, kv_all, start, *extra)


def assemble(axis, first, count, blocks_total, per_dev, me, parts, base):
    n_dev = len(parts)
    other = parts[0].shape[1 - axis]
    last_start = blocks_total - per_dev

    def place(rel, k, me_ref):
        dev = jnp.bitwise_xor(rel, me_ref[0])
        begin = jnp.minimum(dev * per_dev, last_start)
        k = jnp.maximum(k, dev * per_dev - begin - first)
        return k, begin + first + k

    def in_map(i):
        def index(rel, k, me_ref):
            k_here, _ = place(i, k, me_ref)
            k_first, _ = place(i, 0, me_ref)
            k_use = jnp.where(rel == i, k_here, jnp.where(rel < i, k_first, count - 1))
            return (0, k_use) if axis == 1 else (k_use, 0)
        return index

    def out_map(rel, k, me_ref):
        _, dest = place(rel, k, me_ref)
        return (0, dest) if axis == 1 else (dest, 0)

    block = (other, LANE) if axis == 1 else (LANE, other)
    whole = (other, blocks_total * LANE) if axis == 1 else (blocks_total * LANE, other)

    def body(me_ref, *refs):
        out_ref = refs[-1]
        rel = pl.program_id(0)
        for i in range(n_dev):
            @pl.when(rel == i)
            def _(i=i):
                out_ref[...] = refs[i][...]

    in_specs = [pl.BlockSpec(block, in_map(i)) for i in range(n_dev)]
    operands = list(parts)
    aliases = {}
    if base is not None:
        in_specs.append(pl.BlockSpec(memory_space=pl.ANY))
        operands.append(base)
        aliases = {1 + n_dev: 0}
    return pl.pallas_call(
        body,
        grid_spec=pltpu.PrefetchScalarGridSpec(num_scalar_prefetch=1, grid=(n_dev, count), in_specs=in_specs, out_specs=pl.BlockSpec(block, out_map)),
        out_shape=jax.ShapeDtypeStruct(whole, jnp.float32),
        input_output_aliases=aliases,
        compiler_params=pltpu.CompilerParams(vmem_limit_bytes=32 * 1024 * 1024),
        cost_estimate=pl.CostEstimate(flops=30_000_000_000, bytes_accessed=2 * n_dev * count * LANE * other * 4, transcendentals=0),
        name="assemble",
    )(me, *operands)


def solution(mesh):
    dp_size, cp_size = mesh.shape['dp'], mesh.shape['cp']
    workers = dp_size * cp_size
    axes = ('dp', 'cp')

    def pp(value, bit):
        return lax.ppermute(value, axes, [(dev, dev ^ bit) for dev in range(workers)])

    def gather_pair(first, second):
        got_a, got_b = {0: first}, {0: second}
        got_a[2], got_b[4] = pp(first, 2), pp(second, 4)
        got_a[4], got_b[2] = pp(first, 4), pp(second, 2)
        got_a[6], got_b[6] = pp(got_a[2], 4), pp(got_b[4], 2)
        for rel in (0, 2, 4, 6):
            got_a[rel ^ 1], got_b[rel ^ 1] = pp(got_a[rel], 1), pp(got_b[rel], 1)
        return [got_a[rel] for rel in range(8)], [got_b[rel] for rel in range(8)]

    def local_grads(x_loc, dout_loc, seg_loc, w_q, w_k, w_v, w_o, w_up, w_down):
        batch, seq_local, model_width = x_loc.shape
        kv_heads, head_dim = w_k.shape[1], w_k.shape[2]
        heads = w_q.shape[1]
        group = heads // kv_heads
        ffn = w_up.shape[1]
        scale = head_dim ** -0.5
        tokens = batch * seq_local
        cp_index = lax.axis_index('cp')
        me = lax.axis_index(axes)

        x2 = x_loc.reshape(tokens, model_width)
        d2 = dout_loc.reshape(tokens, model_width)
        half = tokens // 2
        dout_a, dout_b = gather_pair(d2[:half], d2[half:])

        wq2 = w_q.reshape(model_width, heads * head_dim)
        wkv2 = jnp.concatenate([w_k.reshape(model_width, -1), w_v.reshape(model_width, -1)], axis=1)
        wo2 = w_o.reshape(heads * head_dim, model_width)

        kv_act = mm(x2, wkv2).astype(jnp.bfloat16).reshape(batch, seq_local, -1)
        kv_all = lax.all_gather(kv_act, 'cp')
        seg_all = lax.all_gather(seg_loc, 'cp')
        start = jnp.sum((seg_all[:, :, None, :] < seg_loc[None, :, :, None]).astype(jnp.int32), axis=(0, 3))
        low = start[:, ::PIECE] // KV_BLOCK
        scal = jnp.concatenate([cp_index.reshape(1).astype(jnp.int32), low.reshape(-1)])
        start3 = start[:, None, :]
        queries = mm(x2, wq2).astype(jnp.bfloat16).reshape(batch, seq_local, -1)

        attn_out, log_norm = attention("forward", cp_size, group, kv_heads, scale, scal, queries, kv_all, start3)
        attn2 = attn_out.reshape(tokens, -1)
        hidden = (x2 + mm(attn2, wo2)).astype(jnp.bfloat16)
        hid_a, hid_b = gather_pair(hidden[:half], hidden[half:])

        up_own = mm(hidden, w_up)
        _, pull_own = jax.vjp(gelu_tanh, up_own)
        d_up_own = pull_own(mm(d2, w_down, NT))[0].astype(jnp.bfloat16)
        d_hidden = d2 + mm(d_up_own, w_up, NT)
        d_hidden_b16 = d_hidden.astype(jnp.bfloat16)
        dw_o = mm(attn2, d_hidden_b16, TN)
        d_attn = mm(d_hidden_b16, wo2, NT).astype(jnp.bfloat16).reshape(batch, seq_local, -1)
        grad_q, part_k, part_v = attention("backward", cp_size, group, kv_heads, scale, scal, queries, kv_all, start3, (attn_out, d_attn, log_norm))
        part_kv = jnp.concatenate([part_k, part_v], axis=3)
        grad_kv = lax.psum_scatter(part_kv, 'cp', scatter_dimension=0).astype(jnp.bfloat16).reshape(tokens, -1)
        grad_q = grad_q.reshape(tokens, -1)
        dw_q = mm(x2, grad_q, TN)
        dw_kv = mm(x2, grad_kv, TN)
        d_x = (d_hidden + mm(grad_q, wq2, NT) + mm(grad_kv, wkv2, NT)).astype(jnp.bfloat16).reshape(x_loc.shape)
        dw_q, dw_kv, dw_o = lax.psum((dw_q / workers, dw_kv / workers, dw_o / workers), axes)
        dw_k, dw_v = jnp.split(dw_kv, 2, axis=1)

        blocks_total = ffn // LANE
        per_dev = -(-blocks_total // workers)
        slice_at = jnp.minimum(me * per_dev, blocks_total - per_dev) * LANE
        hid_all = jnp.concatenate(hid_a + hid_b, axis=0)
        dout_all = jnp.concatenate(dout_a + dout_b, axis=0)
        me_arr = me.reshape(1).astype(jnp.int32)
        dw_up = dw_down = None
        first = 0
        for count in (per_dev - per_dev // 2, per_dev // 2):
            at, wide = slice_at + first * LANE, count * LANE
            up_part = lax.dynamic_slice(w_up, (0, at), (model_width, wide))
            down_part = lax.dynamic_slice(w_down, (at, 0), (wide, model_width))
            up_pre = mm(hid_all, up_part)
            act, pull = jax.vjp(gelu_tanh, up_pre)
            d_up = pull(mm(dout_all, down_part, NT))[0].astype(jnp.bfloat16)
            part_up = mm(hid_all, d_up, TN) / workers
            part_down = mm(act.astype(jnp.bfloat16), dout_all, TN) / workers
            all_up, all_down = gather_pair(part_up, part_down)
            dw_up = assemble(1, first, count, blocks_total, per_dev, me_arr, all_up, dw_up)
            dw_down = assemble(0, first, count, blocks_total, per_dev, me_arr, all_down, dw_down)
            first += count
        return (d_x, dw_q.reshape(w_q.shape), dw_k.reshape(w_k.shape), dw_v.reshape(w_v.shape), dw_o.reshape(w_o.shape), dw_up, dw_down)

    act_spec = P('dp', 'cp', None)
    return jax.shard_map(local_grads, mesh=mesh,
                         in_specs=(act_spec, act_spec, P('dp', 'cp'), P(), P(), P(), P(), P(), P()),
                         out_specs=(act_spec, P(), P(), P(), P(), P(), P()),
                         check_vma=False)
```

```python
import jax
import jax.numpy as jnp
from jax import lax
from jax.experimental import pallas as pl
from jax.experimental.pallas import tpu as pltpu
from jax.sharding import PartitionSpec as P


NEG_BIG = -1e30
PIECE = 128
KV_BLOCK = 256
LANE = 128
GELU_C = 0.7978845608028654
GELU_A = 0.044715


NT = (((1,), (1,)), ((), ()))
NN = (((1,), (0,)), ((), ()))
TN = (((0,), (0,)), ((), ()))


def mm(lhs, rhs, dims=NN):
    return lax.dot_general(lhs, rhs, dims, preferred_element_type=jnp.float32)


def order_pieces(cp_size):
    return [(t, 0) if t < cp_size else (2 * cp_size - 1 - t, 1) for t in range(2 * cp_size)]


def piece_bounds(scal_ref, piece_idx, batch_idx, cp_size):
    cp_index = scal_ref[0]
    piece = cp_index if piece_idx == 0 else 2 * cp_size - 1 - cp_index
    low = scal_ref[1 + 2 * batch_idx + piece_idx]
    return piece, low, (piece + 2) // 2


def block_mask(kv_start, start_row, pos_row):
    kv_pos = kv_start + lax.broadcasted_iota(jnp.int32, (KV_BLOCK, 2 * PIECE), 0)
    return (kv_pos >= start_row) & (kv_pos <= pos_row)


def rows_of(start_ref, piece_idx, piece):
    part = start_ref[0, :, piece_idx * PIECE:(piece_idx + 1) * PIECE]
    start_row = jnp.concatenate([part, part], axis=1)
    pos_row = piece * PIECE + lax.rem(lax.broadcasted_iota(jnp.int32, (1, 2 * PIECE), 1), PIECE)
    return start_row, pos_row


def attn_forward_kernel(cp_size, group, scale, scal_ref, q_ref, k_ref, v_ref, start_ref, o_ref, lse_ref, k_scr, v_scr, q_scr, s_scr, acc_scr):
    batch_idx = pl.program_id(0)
    for t, (dev, half) in enumerate(order_pieces(cp_size)):
        k_scr[t * PIECE:(t + 1) * PIECE, :] = k_ref[dev, 0, half * PIECE:(half + 1) * PIECE, :]
        v_scr[t * PIECE:(t + 1) * PIECE, :] = v_ref[dev, 0, half * PIECE:(half + 1) * PIECE, :]
    width = group * PIECE
    pairs = group // 2
    for piece_idx in range(2):
        piece, low, high = piece_bounds(scal_ref, piece_idx, batch_idx, cp_size)
        rows = slice(piece_idx * PIECE, (piece_idx + 1) * PIECE)
        for head in range(group):
            q_scr[head * PIECE:(head + 1) * PIECE, :] = q_ref[0, rows, head * LANE:(head + 1) * LANE]
        start_row, pos_row = rows_of(start_ref, piece_idx, piece)

        def score_step(blk, row_max):
            at = pl.multiple_of(blk * KV_BLOCK, KV_BLOCK)
            k_blk = k_scr[pl.ds(at, KV_BLOCK), :]
            allowed = block_mask(at, start_row, pos_row)
            new_max = []
            for pair in range(pairs):
                cols = slice(pair * 2 * PIECE, (pair + 1) * 2 * PIECE)
                scores = mm(k_blk, q_scr[cols, :], NT) * scale
                scores = jnp.where(allowed, scores, NEG_BIG)
                s_scr[pl.ds(at, KV_BLOCK), cols] = scores
                new_max.append(jnp.maximum(row_max[pair], jnp.max(scores, axis=0, keepdims=True)))
            return tuple(new_max)

        row_max = lax.fori_loop(low, high, score_step, tuple(jnp.full((1, 2 * PIECE), NEG_BIG, jnp.float32) for _ in range(pairs)))
        acc_scr[...] = jnp.zeros((LANE, width), jnp.float32)

        def value_step(blk, row_sum):
            at = pl.multiple_of(blk * KV_BLOCK, KV_BLOCK)
            v_blk = v_scr[pl.ds(at, KV_BLOCK), :]
            new_sum = []
            for pair in range(pairs):
                cols = slice(pair * 2 * PIECE, (pair + 1) * 2 * PIECE)
                exp_scores = jnp.exp(s_scr[pl.ds(at, KV_BLOCK), cols] - row_max[pair])
                new_sum.append(row_sum[pair] + jnp.sum(exp_scores, axis=0, keepdims=True))
                acc_scr[:, cols] += mm(v_blk, exp_scores.astype(jnp.bfloat16), TN)
            return tuple(new_sum)

        row_sum = lax.fori_loop(low, high, value_step, tuple(jnp.zeros((1, 2 * PIECE), jnp.float32) for _ in range(pairs)))
        for pair in range(pairs):
            cols = slice(pair * 2 * PIECE, (pair + 1) * 2 * PIECE)
            lse_ref[0, 0, piece_idx:piece_idx + 1, cols] = row_max[pair] + jnp.log(row_sum[pair])
            out = jnp.transpose(acc_scr[:, cols] / row_sum[pair]).astype(jnp.bfloat16)
            for side in range(2):
                head = 2 * pair + side
                o_ref[0, rows, head * LANE:(head + 1) * LANE] = out[side * PIECE:(side + 1) * PIECE, :]


def attn_backward_kernel(cp_size, group, scale, scal_ref, q_ref, k_ref, v_ref, start_ref, o_ref, do_ref, lse_ref, dq_ref, dkv_ref,
                         k_scr, v_scr, q_scr, do_scr, dqt_scr, dk_scr, dv_scr):
    batch_idx = pl.program_id(0)
    for t, (dev, half) in enumerate(order_pieces(cp_size)):
        k_scr[t * PIECE:(t + 1) * PIECE, :] = k_ref[dev, 0, half * PIECE:(half + 1) * PIECE, :]
        v_scr[t * PIECE:(t + 1) * PIECE, :] = v_ref[dev, 0, half * PIECE:(half + 1) * PIECE, :]
    dk_scr[...] = jnp.zeros(dk_scr.shape, jnp.float32)
    dv_scr[...] = jnp.zeros(dv_scr.shape, jnp.float32)
    pairs = group // 2
    for piece_idx in range(2):
        piece, low, high = piece_bounds(scal_ref, piece_idx, batch_idx, cp_size)
        rows = slice(piece_idx * PIECE, (piece_idx + 1) * PIECE)
        start_row, pos_row = rows_of(start_ref, piece_idx, piece)
        deltas = []
        for head in range(group):
            lanes = slice(head * LANE, (head + 1) * LANE)
            d_out = do_ref[0, rows, lanes]
            q_scr[head * PIECE:(head + 1) * PIECE, :] = q_ref[0, rows, lanes]
            do_scr[head * PIECE:(head + 1) * PIECE, :] = d_out
            prod = d_out.astype(jnp.float32) * o_ref[0, rows, lanes].astype(jnp.float32)
            deltas.append(jnp.sum(jnp.transpose(prod), axis=0, keepdims=True))
        delta_rows = [jnp.concatenate(deltas[2 * pair:2 * pair + 2], axis=1) for pair in range(pairs)]
        dqt_scr[...] = jnp.zeros(dqt_scr.shape, jnp.float32)

        def step(blk, carry):
            at = pl.multiple_of(blk * KV_BLOCK, KV_BLOCK)
            k_blk = k_scr[pl.ds(at, KV_BLOCK), :]
            v_blk = v_scr[pl.ds(at, KV_BLOCK), :]
            allowed = block_mask(at, start_row, pos_row)
            dk_sum = dk_scr[pl.ds(at, KV_BLOCK), :]
            dv_sum = dv_scr[pl.ds(at, KV_BLOCK), :]
            for pair in range(pairs):
                cols = slice(pair * 2 * PIECE, (pair + 1) * 2 * PIECE)
                q_pair = q_scr[cols, :]
                do_pair = do_scr[cols, :]
                scores = mm(k_blk, q_pair, NT) * scale
                prob = jnp.where(allowed, jnp.exp(scores - lse_ref[0, 0, piece_idx:piece_idx + 1, cols]), 0.0)
                d_prob = mm(v_blk, do_pair, NT)
                d_score = (prob * (d_prob - delta_rows[pair]) * scale).astype(jnp.bfloat16)
                dv_sum = dv_sum + mm(prob.astype(jnp.bfloat16), do_pair)
                dk_sum = dk_sum + mm(d_score, q_pair)
                dqt_scr[:, cols] += mm(k_blk, d_score, TN)
            dk_scr[pl.ds(at, KV_BLOCK), :] = dk_sum
            dv_scr[pl.ds(at, KV_BLOCK), :] = dv_sum
            return carry

        lax.fori_loop(low, high, step, 0)
        for pair in range(pairs):
            cols = slice(pair * 2 * PIECE, (pair + 1) * 2 * PIECE)
            d_q = jnp.transpose(dqt_scr[:, cols]).astype(jnp.bfloat16)
            for side in range(2):
                head = 2 * pair + side
                dq_ref[0, rows, head * LANE:(head + 1) * LANE] = d_q[side * PIECE:(side + 1) * PIECE, :]
    k_lane = pl.multiple_of(pl.program_id(1) * LANE, LANE)
    v_lane = pl.multiple_of((pl.num_programs(1) + pl.program_id(1)) * LANE, LANE)
    for t, (dev, half) in enumerate(order_pieces(cp_size)):
        place = slice(half * PIECE, (half + 1) * PIECE)
        dkv_ref[dev, 0, place, pl.ds(k_lane, LANE)] = dk_scr[t * PIECE:(t + 1) * PIECE, :]
        dkv_ref[dev, 0, place, pl.ds(v_lane, LANE)] = dv_scr[t * PIECE:(t + 1) * PIECE, :]


def attention(mode, cp_size, group, kv_heads, scale, scal, queries, kv_all, start, extra=()):
    batch, seq_local, _ = queries.shape
    seq_len = cp_size * seq_local
    gw = group * LANE
    kernel = attn_forward_kernel if mode == "forward" else attn_backward_kernel
    q_spec = pl.BlockSpec((1, seq_local, gw), lambda b, n, s: (b, 0, n))
    k_spec = pl.BlockSpec((cp_size, 1, seq_local, LANE), lambda b, n, s: (0, b, 0, n))
    v_spec = pl.BlockSpec((cp_size, 1, seq_local, LANE), lambda b, n, s: (0, b, 0, kv_heads + n))
    start_spec = pl.BlockSpec((1, 1, seq_local), lambda b, n, s: (b, 0, 0))
    lse_spec = pl.BlockSpec((1, 1, 2, group * PIECE), lambda b, n, s: (b, n, 0, 0))
    act_shape = jax.ShapeDtypeStruct(queries.shape, jnp.bfloat16)
    bf = jnp.bfloat16
    f32 = jnp.float32
    flops = 2 * batch * kv_heads * group * seq_local * (seq_len // 2 + PIECE) * LANE
    if mode == "forward":
        in_specs = [q_spec, k_spec, v_spec, start_spec]
        out_specs = [q_spec, lse_spec]
        out_shape = [act_shape, jax.ShapeDtypeStruct((batch, kv_heads, 2, group * PIECE), f32)]
        scratch = [pltpu.VMEM((seq_len, LANE), bf), pltpu.VMEM((seq_len, LANE), bf), pltpu.VMEM((group * PIECE, LANE), bf),
                   pltpu.VMEM((seq_len, group * PIECE), f32), pltpu.VMEM((LANE, group * PIECE), f32)]
        flops = 4 * flops
    else:
        in_specs = [q_spec, k_spec, v_spec, start_spec, q_spec, q_spec, lse_spec]
        out_specs = [q_spec, pl.BlockSpec((cp_size, 1, seq_local, 2 * kv_heads * LANE), lambda b, n, s: (0, b, 0, 0))]
        out_shape = [act_shape, jax.ShapeDtypeStruct((cp_size, batch, seq_local, 2 * kv_heads * LANE), f32)]
        scratch = [pltpu.VMEM((seq_len, LANE), bf), pltpu.VMEM((seq_len, LANE), bf), pltpu.VMEM((group * PIECE, LANE), bf),
                   pltpu.VMEM((group * PIECE, LANE), bf), pltpu.VMEM((LANE, group * PIECE), f32),
                   pltpu.VMEM((seq_len, LANE), f32), pltpu.VMEM((seq_len, LANE), f32)]
        flops = 8 * flops

    def body(*refs):
        kernel(cp_size, group, scale, *refs)

    return pl.pallas_call(
        body,
        grid_spec=pltpu.PrefetchScalarGridSpec(num_scalar_prefetch=1, grid=(batch, kv_heads), in_specs=in_specs, out_specs=out_specs, scratch_shapes=scratch),
        out_shape=out_shape,
        compiler_params=pltpu.CompilerParams(vmem_limit_bytes=48 * 1024 * 1024),
        cost_estimate=pl.CostEstimate(flops=flops, bytes_accessed=40 * 1024 * 1024, transcendentals=flops // 512),
    )(scal, queries, kv_all, kv_all, start, *extra)


def dual_rows(sub_rows, h_ref, d_ref, up_ref, down_ref, out_refs):
    up_w, down_w = up_ref[...], down_ref[...]
    for at in range(0, h_ref.shape[0], sub_rows):
        rows = slice(at, at + sub_rows)
        pre = mm(h_ref[rows, :], up_w)
        d_act = mm(d_ref[rows, :], down_w, NT)
        square = pre * pre
        half_tanh = 0.5 * jnp.tanh(GELU_C * pre * (1.0 + GELU_A * square))
        gate = 0.5 + half_tanh
        slope = gate + pre * (0.5 - 2.0 * half_tanh * half_tanh) * (GELU_C * (1.0 + 3.0 * GELU_A * square))
        if len(out_refs) > 1:
            out_refs[1][rows, :] = (pre * gate).astype(jnp.bfloat16)
        out_refs[0][rows, :] = (d_act * slope).astype(jnp.bfloat16)


def dual_gather(h_parts, d_parts, up_w, down_w, tile_rows, sub_rows, ahead):
    n_parts = len(h_parts)
    part_rows, width = h_parts[0].shape
    cols = up_w.shape[1]
    per_part = part_rows // tile_rows
    steps = n_parts * per_part
    rows = steps * tile_rows
    slots = 3

    def body(*refs):
        h_refs, d_refs = refs[:n_parts], refs[n_parts:2 * n_parts]
        up_ref, down_ref = refs[2 * n_parts:2 * n_parts + 2]
        dup_ref, act_ref, h_all, d_all, h_scr, d_scr, in_sem, out_sem = refs[2 * n_parts + 2 + len(ahead):]
        step = pl.program_id(0)

        def load(idx):
            slot = lax.rem(idx, slots)
            at = pl.multiple_of(lax.rem(idx, per_part) * tile_rows, tile_rows)
            for part in range(n_parts):
                @pl.when(idx // per_part == part)
                def _(part=part):
                    pltpu.make_async_copy(h_refs[part].at[pl.ds(at, tile_rows)], h_scr.at[slot], in_sem.at[0, slot]).start()
                    pltpu.make_async_copy(d_refs[part].at[pl.ds(at, tile_rows)], d_scr.at[slot], in_sem.at[1, slot]).start()

        def stores(idx):
            slot = lax.rem(idx, slots)
            at = pl.multiple_of(idx * tile_rows, tile_rows)
            return (pltpu.make_async_copy(h_scr.at[slot], h_all.at[pl.ds(at, tile_rows)], out_sem.at[0, slot]),
                    pltpu.make_async_copy(d_scr.at[slot], d_all.at[pl.ds(at, tile_rows)], out_sem.at[1, slot]))

        @pl.when(step == 0)
        def _():
            load(step)

        @pl.when(step >= 2)
        def _():
            for copy in stores(step - 2):
                copy.wait()

        @pl.when(step + 1 < steps)
        def _():
            load(step + 1)

        slot = lax.rem(step, slots)
        pltpu.make_async_copy(h_refs[0].at[pl.ds(0, tile_rows)], h_scr.at[slot], in_sem.at[0, slot]).wait()
        pltpu.make_async_copy(d_refs[0].at[pl.ds(0, tile_rows)], d_scr.at[slot], in_sem.at[1, slot]).wait()
        for copy in stores(step):
            copy.start()
        dual_rows(sub_rows, h_scr.at[slot], d_scr.at[slot], up_ref, down_ref, (dup_ref, act_ref))

        @pl.when(step == steps - 1)
        def _():
            for copy in stores(step - 1) + stores(step):
                copy.wait()

    bf = jnp.bfloat16
    any_spec = pl.BlockSpec(memory_space=pl.ANY)
    out_spec = pl.BlockSpec((tile_rows, cols), lambda i: (i, 0))
    whole = jax.ShapeDtypeStruct((rows, width), bf)
    out = jax.ShapeDtypeStruct((rows, cols), bf)
    return pl.pallas_call(
        body,
        grid=(steps,),
        in_specs=[any_spec] * (2 * n_parts) + [pl.BlockSpec((width, cols), lambda i: (0, 0)), pl.BlockSpec((cols, width), lambda i: (0, 0))] + [any_spec] * len(ahead),
        out_specs=[out_spec, out_spec, any_spec, any_spec],
        out_shape=[out, out, whole, whole],
        scratch_shapes=[pltpu.VMEM((slots, tile_rows, width), bf), pltpu.VMEM((slots, tile_rows, width), bf),
                        pltpu.SemaphoreType.DMA((2, slots)), pltpu.SemaphoreType.DMA((2, slots))],
        compiler_params=pltpu.CompilerParams(vmem_limit_bytes=60 * 1024 * 1024, dimension_semantics=("arbitrary",)),
        cost_estimate=pl.CostEstimate(flops=4 * rows * cols * width, bytes_accessed=4 * rows * (cols + 2 * width), transcendentals=rows * cols),
        name="dual_gather",
    )(*h_parts, *d_parts, up_w, down_w, *ahead)


def dual(h_in, d_in, up_w, down_w, tile_rows, tile_cols, sub_rows, with_act):
    rows, width = h_in.shape
    cols = up_w.shape[1]
    out = jax.ShapeDtypeStruct((rows, cols), jnp.bfloat16)
    n_out = 2 if with_act else 1

    def body(h_ref, d_ref, up_ref, down_ref, *out_refs):
        dual_rows(sub_rows, h_ref, d_ref, up_ref, down_ref, out_refs)

    act_spec = pl.BlockSpec((tile_rows, width), lambda i, j: (i, 0))
    out_spec = pl.BlockSpec((tile_rows, tile_cols), lambda i, j: (i, j))
    return pl.pallas_call(
        body,
        grid=(rows // tile_rows, cols // tile_cols),
        in_specs=[act_spec, act_spec, pl.BlockSpec((width, tile_cols), lambda i, j: (0, j)), pl.BlockSpec((tile_cols, width), lambda i, j: (j, 0))],
        out_specs=[out_spec] * n_out,
        out_shape=[out] * n_out,
        compiler_params=pltpu.CompilerParams(vmem_limit_bytes=56 * 1024 * 1024),
        cost_estimate=pl.CostEstimate(flops=4 * rows * cols * width, bytes_accessed=4 * rows * (cols + width), transcendentals=rows * cols),
        name="dual",
    )(h_in, d_in, up_w, down_w)


def assemble(axis, first, count, blocks_total, per_dev, me, parts, base, rel_first):
    n_dev = len(parts)
    other = parts[0].shape[1 - axis]
    last_start = blocks_total - per_dev

    def place(rel, k, me_ref):
        dev = jnp.bitwise_xor(rel + rel_first, me_ref[0])
        begin = jnp.minimum(dev * per_dev, last_start)
        k = jnp.maximum(k, dev * per_dev - begin - first)
        return k, begin + first + k

    def in_map(i):
        def index(rel, k, me_ref):
            k_here, _ = place(i, k, me_ref)
            k_first, _ = place(i, 0, me_ref)
            k_use = jnp.where(rel == i, k_here, jnp.where(rel < i, k_first, count - 1))
            return (0, k_use) if axis == 1 else (k_use, 0)

        return index

    def out_map(rel, k, me_ref):
        _, dest = place(rel, k, me_ref)
        return (0, dest) if axis == 1 else (dest, 0)

    block = (other, LANE) if axis == 1 else (LANE, other)
    whole = (other, blocks_total * LANE) if axis == 1 else (blocks_total * LANE, other)

    def body(me_ref, *refs):
        out_ref = refs[-1]
        rel = pl.program_id(0)
        for i in range(n_dev):
            @pl.when(rel == i)
            def _(i=i):
                out_ref[...] = refs[i][...]

    in_specs = [pl.BlockSpec(block, in_map(i)) for i in range(n_dev)]
    operands = list(parts)
    aliases = {}
    if base is not None:
        in_specs.append(pl.BlockSpec(memory_space=pl.ANY))
        operands.append(base)
        aliases = {1 + n_dev: 0}
    return pl.pallas_call(
        body,
        grid_spec=pltpu.PrefetchScalarGridSpec(num_scalar_prefetch=1, grid=(n_dev, count), in_specs=in_specs, out_specs=pl.BlockSpec(block, out_map)),
        out_shape=jax.ShapeDtypeStruct(whole, jnp.float32),
        input_output_aliases=aliases,
        compiler_params=pltpu.CompilerParams(vmem_limit_bytes=32 * 1024 * 1024),
        cost_estimate=pl.CostEstimate(flops=5_000_000_000 * n_dev, bytes_accessed=2 * n_dev * count * LANE * other * 4, transcendentals=0),
        name="assemble",
    )(me, *operands)


def solution(mesh):
    dp_size, cp_size = mesh.shape['dp'], mesh.shape['cp']
    workers = dp_size * cp_size
    axes = ('dp', 'cp')

    def pp(value, bit):
        return lax.ppermute(value, axes, [(dev, dev ^ bit) for dev in range(workers)])

    def phase_one(first, second):
        got_a = {0: first, 4: pp(first, 4), 2: pp(first, 2), 1: pp(first, 1)}
        got_b = {0: second, 4: pp(second, 4), 2: pp(second, 2), 1: pp(second, 1)}
        return got_a, got_b

    def phase_two(got_a, got_b):
        got_a[6], got_b[6] = pp(got_a[2], 4), pp(got_b[4], 2)
        got_a.update({3: pp(got_a[2], 1), 5: pp(got_a[4], 1)})
        got_b.update({3: pp(got_b[2], 1), 5: pp(got_b[4], 1)})

    def phase_three(got_a, got_b):
        got_a[7], got_b[7] = pp(got_a[6], 1), pp(got_b[6], 1)

    def listed(got, rels):
        return [got[rel] for rel in rels]

    def local_grads(x_loc, dout_loc, seg_loc, w_q, w_k, w_v, w_o, w_up, w_down):
        batch, seq_local, model_width = x_loc.shape
        kv_heads, head_dim = w_k.shape[1], w_k.shape[2]
        heads = w_q.shape[1]
        group = heads // kv_heads
        ffn = w_up.shape[1]
        scale = head_dim ** -0.5
        tokens = batch * seq_local
        cp_index = lax.axis_index('cp')
        me = lax.axis_index(axes)
        me_arr = me.reshape(1).astype(jnp.int32)
        everyone = range(workers)

        x2 = x_loc.reshape(tokens, model_width)
        d2 = dout_loc.reshape(tokens, model_width)
        half = tokens // 2

        wq2 = w_q.reshape(model_width, heads * head_dim)
        wkv2 = jnp.concatenate([w_k.reshape(model_width, -1), w_v.reshape(model_width, -1)], axis=1)
        wo2 = w_o.reshape(heads * head_dim, model_width)

        seg_all = lax.all_gather(seg_loc, 'cp')
        kv_act = mm(x2, wkv2).astype(jnp.bfloat16).reshape(batch, seq_local, -1)
        kv_all = lax.all_gather(kv_act, 'cp')
        dout_a, dout_b = phase_one(d2[:half], d2[half:])
        start = jnp.sum((seg_all[:, :, None, :] < seg_loc[None, :, :, None]).astype(jnp.int32), axis=(0, 3))
        low = start[:, ::PIECE] // KV_BLOCK
        scal = jnp.concatenate([cp_index.reshape(1).astype(jnp.int32), low.reshape(-1)])
        start3 = start[:, None, :]
        queries = mm(x2, wq2).astype(jnp.bfloat16).reshape(batch, seq_local, -1)

        attn_out, log_norm = attention("forward", cp_size, group, kv_heads, scale, scal, queries, kv_all, start3)
        attn2 = attn_out.reshape(tokens, -1)
        hidden = (x2 + mm(attn2, wo2)).astype(jnp.bfloat16)
        hid_a, hid_b = phase_one(hidden[:half], hidden[half:])

        d_up_own, = dual(hidden, d2, w_up, w_down, 1024, 256, 256, False)
        phase_two(dout_a, dout_b)
        d_hidden = d2 + mm(d_up_own, w_up, NT)
        d_hidden_b16 = d_hidden.astype(jnp.bfloat16)
        d_attn = mm(d_hidden_b16, wo2, NT).astype(jnp.bfloat16).reshape(batch, seq_local, -1)
        phase_two(hid_a, hid_b)
        phase_three(dout_a, dout_b)
        grad_q, part_kv = attention("backward", cp_size, group, kv_heads, scale, scal, queries, kv_all, start3, (attn_out, d_attn, log_norm))
        phase_three(hid_a, hid_b)
        grad_kv = lax.psum_scatter(part_kv, 'cp', scatter_dimension=0).astype(jnp.bfloat16).reshape(tokens, -1)
        grad_q = grad_q.reshape(tokens, -1)
        dw_o = mm(attn2, d_hidden_b16, TN) / workers
        dw_q = mm(x2, grad_q, TN) / workers
        dw_kv = mm(x2, grad_kv, TN) / workers
        ahead = [part[:8, :LANE] for part in (dw_o, dw_q, dw_kv)]
        dw_q, dw_kv, dw_o = lax.psum((dw_q, dw_kv, dw_o), axes)
        dw_q, dw_kv, dw_o = lax.optimization_barrier((dw_q, dw_kv, dw_o))
        dw_k, dw_v = jnp.split(dw_kv, 2, axis=1)

        blocks_total = ffn // LANE
        per_dev = -(-blocks_total // workers)
        slice_at = jnp.minimum(me * per_dev, blocks_total - per_dev) * LANE
        hid_all = dout_all = None
        chunks, first = [], 0
        for count in (per_dev - per_dev // 2, per_dev // 2):
            at, wide = slice_at + first * LANE, count * LANE
            up_part = lax.dynamic_slice(w_up, (0, at), (model_width, wide))
            down_part = lax.dynamic_slice(w_down, (at, 0), (wide, model_width))
            if hid_all is None:
                d_up, act, hid_all, dout_all = dual_gather(listed(hid_a, everyone) + listed(hid_b, everyone), listed(dout_a, everyone) + listed(dout_b, everyone), up_part, down_part, 512, 256, ahead)
            else:
                d_up, act = dual(hid_all, dout_all, up_part, down_part, 512, wide, 256, True)
            part_up = mm(hid_all, d_up, TN) / workers
            part_down = mm(act, dout_all, TN) / workers
            got = phase_one(part_up, part_down)
            chunks.append((first, count, got))
            first += count
        d_x = (d_hidden + mm(grad_q, wq2, NT) + mm(grad_kv, wkv2, NT)).astype(jnp.bfloat16).reshape(x_loc.shape)
        sums = [None, None]
        for first, count, got in chunks:
            phase_two(*got)
            phase_three(*got)
            for rel_first, rels in ((0, range(6)), (6, range(6, 8))):
                for which in range(2):
                    sums[which] = assemble(1 - which, first, count, blocks_total, per_dev, me_arr, listed(got[which], rels), sums[which], rel_first)
        return (d_x, dw_q.reshape(w_q.shape), dw_k.reshape(w_k.shape), dw_v.reshape(w_v.shape), dw_o.reshape(w_o.shape), sums[0], sums[1])

    act_spec = P('dp', 'cp', None)

    return jax.shard_map(local_grads, mesh=mesh,
                         in_specs=(act_spec, act_spec, P('dp', 'cp'), P(), P(), P(), P(), P(), P()),
                         out_specs=(act_spec, P(), P(), P(), P(), P(), P()),
                         check_vma=False)
```
